32 devices in a mesh: dp: 16 (over z, y, x), expert: 2 (over core).
Axes of the slice: x: 2, y: 2, z: 4, core: 2. Of those that a mesh axis runs over, the one named last changes fastest.
Arguments:
- master: float32 [2, 7168, 2048], P('expert', 'dp'), may hold values from -6 to 6
- first_moment: float32 [2, 7168, 2048], P('expert', 'dp'), may hold values from -0.06 to 0.06
- second_moment: float32 [2, 7168, 2048], P('expert', 'dp'), may hold values from 1e-05 to 0.001
- rotation: int32 [4, 16, 1], replicated, may hold values from 0 to 15; in each aligned block of 16 rows (0 to 15, 16 to 31, ..., all dimensions but the last counted through in order) at most 3 rows name the same one
- assignment: int32 [64], replicated, may hold values from 0 to 63, each once
Outputs:
- saved_master: float32 [2, 64, 3, 1792, 128], P('expert', 'dp')
- saved_update: float32 [2, 64, 3, 1792, 128], P('expert', 'dp')
- checksums: float32 [2, 2, 64], replicated
The draws below stay inside these ranges and needn't reach their ends.
Inputs may be any that keep to these rules, and one draw needn't show every extreme that they name: rotation[r, j, 0] is the dp index that writes span j of round r; within one round no index is named more than 3 times, and in some round one index is named exactly 3 times. `assignment`: a permutation of the spans' checksum slots.
All inputs are finite; a program needn't handle non-finite values.
Results may differ from the reference program's by a relative error of at most 0.00002.
Values sent between devices are 32-bit elements; how exact they have to be, the bound alone decides.
A program may use at most 128 MiB of HBM per device.

```python
import math
import jax
import jax.numpy as jnp
import numpy as np
from jax import lax

ROWS = 7168
COLS = 2048
LANE = 128
ROUNDS = 4
MOST = 3
STEP = 20
GROUPS = 2
SPANS = 64
N_DP = 16


def block_levels(stream_key, shape, pieces, smallest, top_value):
    gain, own = 1.0, jax.random.fold_in(stream_key, 6)
    for position, blocks in pieces:
        draws = jnp.exp(jax.random.uniform(jax.random.fold_in(own, position), (blocks,), jnp.float32, smallest / len(pieces), top_value / len(pieces)))
        gain = gain * jnp.repeat(draws, shape[position] // blocks).reshape([-1 if axis == position else 1 for axis in range(len(shape))])
    return gain


def shared_out(key, own, number, rows, count, top, bound, slope):
    ranking = jax.random.permutation(key, count)
    packed, usual = shares(count, rows * top, bound, slope, True), shares(count, rows * top, bound, slope, False)
    places = jnp.arange(count)

    def named(tallies, turn):
        used = int((tallies > 0).sum())
        fixed = max(1, used // 4)
        shifted = fixed + (places - fixed + turn * (used - fixed)) % max(1, count - fixed)
        return jnp.zeros((count,), jnp.int32).at[ranking[jnp.where(places < fixed, places, shifted)]].set(jnp.asarray(tallies, jnp.int32))

    tallies = jnp.where(number % 4 == 0, named(packed, number // 4), named(usual, number - number // 4 - 1))
    mixed = jax.random.permutation(jax.random.fold_in(own, 3), count)
    donor, sink = mixed[0:count // 2 * 2:2], mixed[1:count // 2 * 2:2]
    slack = jnp.minimum(tallies[donor] - 1, bound - tallies[sink]) // 2
    slack = jnp.where((donor == ranking[0]) | (sink == ranking[0]) | (tallies[sink] == 0), 0, jnp.maximum(slack, 0))
    shifted = jax.random.randint(jax.random.fold_in(own, 4), (count // 2,), 0, 1 << 20) % (slack + 1)
    tallies = tallies.at[donor].add(-shifted).at[sink].add(shifted)
    items = jnp.searchsorted(jnp.cumsum(tallies), jnp.arange(rows * top), side="right").astype(jnp.int32)
    listing = items.reshape(top, rows).T
    listing = listing[jax.random.permutation(jax.random.fold_in(own, 1), rows)]
    turn = jax.random.randint(jax.random.fold_in(own, 2), (rows, 1), 0, top)
    return jnp.take_along_axis(listing, (jnp.arange(top)[None, :] + turn) % top, axis=1)


def shares(amount, total, reach, slope, full):
    weights = [(1 << 20) // math.isqrt(standing ** slope) + 1 for standing in range(1, amount + 1)]
    largest = reach if full else min(reach, max(-(-total // amount), total * weights[0] // sum(weights)))
    least = 1 if total - largest >= amount - 1 else 0
    holding, rest = [largest] + [least] * (amount - 1), total - largest - least * (amount - 1)
    while rest > 0:
        movable = [i for i in range(1, amount) if holding[i] < largest] or [i for i in range(1, amount) if holding[i] < reach]
        whole, remaining = sum([weights[i] for i in movable]), rest
        for i in movable:
            extra = min(reach - holding[i], max(1, remaining * weights[i] // whole), rest)
            holding[i] = holding[i] + extra
            rest = rest - extra
    return np.array(holding)


def normal_values(rng, extent, deviation, reach, pieces=(), held_as=jnp.bfloat16):
    factor_of = block_levels(rng, extent, pieces, -0.22, 0.18) if pieces else 1.0
    drawn = jax.random.normal(rng, extent, jnp.float32) * deviation * factor_of
    return jnp.minimum(jnp.maximum(drawn, -reach), reach).astype(held_as)


def setup_inputs(seed: int = 0) -> dict:
    streams_of = jax.random.split(jax.random.key(seed), 6)
    master = normal_values(streams_of[0], (GROUPS, ROWS, COLS), 1.0, 6.0, ((0, 2), (1, 16)), jnp.float32)
    first_moment = normal_values(streams_of[1], (GROUPS, ROWS, COLS), 0.01, 0.06, ((0, 2), (1, 16)), jnp.float32)
    second_moment = jnp.clip(jnp.exp(math.log(0.001) - 4.6051703 * jax.random.uniform(streams_of[2], (GROUPS, ROWS, COLS), jnp.float32) ** block_levels(streams_of[2], (GROUPS, ROWS, COLS), ((0, 2), (1, 16)), -0.2, 0.2)), 9.999999747378752e-06, 0.001)
    rotation_keys = jax.random.split(jax.random.fold_in(streams_of[3], 1), ROUNDS * N_DP // N_DP)
    rotation_turns = jax.random.permutation(jax.random.fold_in(streams_of[3], 3), ROUNDS * N_DP // N_DP)
    rotation = jax.vmap(lambda own, number: shared_out(jax.random.fold_in(streams_of[3], 2), own, number, N_DP, N_DP, 1, MOST, 2))(rotation_keys, rotation_turns).reshape((ROUNDS, N_DP, 1))
    assignment = jax.random.permutation(streams_of[4], SPANS).astype(jnp.int32)
    return {"master": master, "first_moment": first_moment, "second_moment": second_moment, "rotation": rotation, "assignment": assignment}


BETA_ONE = 0.9
BETA_TWO = 0.95
EPSILON = 1e-08

def scaled_moment(first_part, second_part):
    corr_one = 1.0 - BETA_ONE ** STEP
    corr_two = 1.0 - BETA_TWO ** STEP
    return first_part / corr_one / (jnp.sqrt(second_part / corr_two) + EPSILON)

def slot_table(rotation, dp_count, most_slots):
    owners = rotation[:, :, 0]
    span_ids = jnp.arange(dp_count, dtype=jnp.int32)
    same_writer = owners[:, :, None] == owners[:, None, :]
    before = span_ids[None, :] < span_ids[:, None]
    slot_rank = lax.optimization_barrier(jnp.sum((same_writer & before[None]).astype(jnp.int32), axis=2))
    writers = jnp.arange(dp_count, dtype=jnp.int32)
    slot_ids = jnp.arange(most_slots, dtype=jnp.int32)
    matches = (owners[:, None, None, :] == writers[None, None, :, None]) & (slot_rank[:, None, None, :] == slot_ids[None, :, None, None])
    matches = matches.astype(jnp.int32)
    found_any = lax.optimization_barrier(jnp.sum(matches, axis=3))
    picked = lax.optimization_barrier(jnp.sum(matches * span_ids, axis=3))
    return (picked + (1 - found_any) * dp_count).astype(jnp.int32)

def position_weights(line_ids, per_row, lane_count):
    row_ids = line_ids // per_row
    col_ids = line_ids % per_row * lane_count
    lane_ids = jnp.arange(lane_count, dtype=jnp.int32)
    pattern = (row_ids[..., None] * 5 + (col_ids[..., None] + lane_ids) * 3) % 11
    return 1.0 + pattern.astype(jnp.float32) / 10.0

def reference(master, first_moment, second_moment, rotation, assignment):
    per_row = COLS // LANE
    lines_device = ROWS // N_DP * per_row
    piece_len = lines_device // (ROUNDS * N_DP)
    inv_count = 1.0 / math.sqrt(N_DP * piece_len * LANE)
    table = slot_table(rotation, N_DP, MOST)
    line_ids = jnp.arange(ROWS * per_row, dtype=jnp.int32).reshape(N_DP, ROUNDS, N_DP, piece_len)
    weights = position_weights(line_ids, per_row, LANE)
    round_ids = jnp.arange(ROUNDS, dtype=jnp.int32)[:, None, None]

    def arrange_field(field_in):
        line_view = field_in.reshape(N_DP, ROUNDS, N_DP, piece_len, LANE)
        totals = lax.optimization_barrier(jnp.sum(line_view * weights, axis=(0, 3, 4))) * inv_count
        reordered = jnp.transpose(line_view, (1, 2, 0, 3, 4))
        padded = jnp.concatenate([reordered, jnp.zeros((ROUNDS, 1, N_DP, piece_len, LANE), reordered.dtype)], axis=1)
        selected = padded[round_ids, table]
        saved_rows = jnp.transpose(selected, (2, 0, 1, 3, 4, 5)).reshape(N_DP * ROUNDS, MOST, N_DP * piece_len, LANE)
        return (saved_rows, totals.reshape(ROUNDS * N_DP))

    def one_group(fields):
        master_part, first_part, second_part = fields
        update = scaled_moment(first_part, second_part)
        saved_master, master_sums = arrange_field(master_part)
        saved_update, update_sums = arrange_field(update)
        return (saved_master, saved_update, jnp.stack([master_sums, update_sums]))
    saved_master, saved_update, group_sums = lax.map(one_group, (master, first_moment, second_moment))
    checksums = jnp.zeros_like(group_sums).at[:, :, assignment.astype(jnp.int32)].set(group_sums)
    return (saved_master, saved_update, checksums)
```

```python
import functools
import math

import jax
import jax.numpy as jnp
from jax import lax
from jax.experimental import pallas as pl
from jax.experimental.pallas import tpu as pltpu
from jax.sharding import PartitionSpec as P

LANE = 128
MOST = 3
STEP = 20
INNER = 4


BETA_ONE = 0.9
BETA_TWO = 0.95
EPSILON = 1e-08


def scaled_moment(first_part, second_part):
    corr_one = 1.0 - BETA_ONE**STEP
    corr_two = 1.0 - BETA_TWO**STEP
    return first_part / corr_one / (jnp.sqrt(second_part / corr_two) + EPSILON)


def slot_table(rotation, dp_count, most_slots):
    owners = rotation[:, :, 0]
    span_ids = jnp.arange(dp_count, dtype=jnp.int32)
    same_writer = owners[:, :, None] == owners[:, None, :]
    before = span_ids[None, :] < span_ids[:, None]
    slot_rank = jnp.sum((same_writer & before[None]).astype(jnp.int32), axis=2)
    writers = jnp.arange(dp_count, dtype=jnp.int32)
    slot_ids = jnp.arange(most_slots, dtype=jnp.int32)
    matches = (owners[:, None, None, :] == writers[None, None, :, None]) & (
        slot_rank[:, None, None, :] == slot_ids[None, :, None, None]
    )
    matches = matches.astype(jnp.int32)
    found_any = jnp.sum(matches, axis=3)
    picked = jnp.sum(matches * span_ids, axis=3)
    return picked + (1 - found_any) * dp_count


def position_weights(line_ids, per_row, lane_count):
    row_ids = line_ids // per_row
    col_ids = line_ids % per_row * lane_count
    lane_ids = jnp.arange(lane_count, dtype=jnp.int32)
    pattern = (row_ids[..., None] * 5 + (col_ids[..., None] + lane_ids) * 3) % 11
    return 1.0 + pattern.astype(jnp.float32) / 10.0


def exchange_kernel(planes, inner, slots, cap, pos_ref, m_ref, u_ref, om_ref, ou_ref, *scratch):
    held = scratch[: 2 * planes]
    stage = scratch[2 * planes : 4 * planes]
    zs_sem, zr_sem, local_sem, is_sem, ir_sem, self_sem = scratch[4 * planes :]
    me = lax.axis_index("dp")
    plane = me // inner
    spot = me % inner
    core = lax.axis_index("expert")
    fields = (m_ref, u_ref)
    outs = (om_ref, ou_ref)

    def peer(plane_to, spot_to):
        return (plane_to * inner + spot_to, core)

    barrier = pltpu.get_barrier_semaphore()
    for d in range(1, planes):
        pl.semaphore_signal(
            barrier, inc=1, device_id=peer((plane + d) % planes, spot), device_id_type=pl.DeviceIdType.MESH
        )
    for e in range(1, inner):
        pl.semaphore_signal(
            barrier, inc=1, device_id=peer(plane, (spot + e) % inner), device_id_type=pl.DeviceIdType.MESH
        )
    pl.semaphore_wait(barrier, planes + inner - 2)

    far = [None] * (2 * planes)
    for f in range(2):
        own = pltpu.make_async_copy(fields[f].at[plane], held[f * planes], local_sem.at[f])
        own.start()
        far[f * planes] = own
        for d in range(1, planes):
            to_plane = (plane + d) % planes
            copy = pltpu.make_async_remote_copy(
                src_ref=fields[f].at[to_plane],
                dst_ref=held[f * planes + d],
                send_sem=zs_sem.at[f * planes + d],
                recv_sem=zr_sem.at[f * planes + d],
                device_id=peer(to_plane, spot),
                device_id_type=pl.DeviceIdType.MESH,
            )
            copy.start()
            far[f * planes + d] = copy

    near = []
    for f in range(2):
        for d in range(planes):
            g = f * planes + d
            if d == 0:
                far[g].wait()
            else:
                far[g].wait_recv()

            def place(t, carry, g=g):
                e = t // slots
                s = t % slots
                index = pos_ref[(spot + e) % inner, s]
                found = index < cap
                lines = held[g][jnp.where(found, index, 0)]
                stage[g][e, s] = jnp.where(found, lines, 0.0)
                return carry

            lax.fori_loop(0, inner * slots, place, 0)
            source = ((plane + planes - d) % planes) * inner + spot
            for e in range(1, inner):
                copy = pltpu.make_async_remote_copy(
                    src_ref=stage[g].at[e],
                    dst_ref=outs[f].at[:, source],
                    send_sem=is_sem.at[g * inner + e],
                    recv_sem=ir_sem.at[g * inner + e],
                    device_id=peer(plane, (spot + e) % inner),
                    device_id_type=pl.DeviceIdType.MESH,
                )
                copy.start()
                near.append(copy)
            copy = pltpu.make_async_copy(stage[g].at[0], outs[f].at[:, source], self_sem.at[g])
            copy.start()
            near.append(copy)
    for f in range(2):
        for d in range(1, planes):
            far[f * planes + d].wait_send()
    for copy in near:
        copy.wait()


def exchange(planes, inner, slots, cap, branch, positions, master_send, update_send):
    lines, lanes = master_send.shape[2:]
    shape = jax.ShapeDtypeStruct((slots, planes * inner, lines, lanes), jnp.float32)
    any_space = pl.BlockSpec(memory_space=pl.ANY)
    steps = 2 * planes
    sent = (planes - 1) * cap * 2 * lines * lanes * 4
    return pl.pallas_call(
        functools.partial(exchange_kernel, planes, inner, slots, cap),
        out_shape=(shape, shape),
        in_specs=[pl.BlockSpec(memory_space=pltpu.SMEM), any_space, any_space],
        out_specs=(any_space, any_space),
        scratch_shapes=[pltpu.VMEM((cap, lines, lanes), jnp.float32)] * steps
        + [pltpu.VMEM((inner, slots, lines, lanes), jnp.float32)] * steps
        + [
            pltpu.SemaphoreType.DMA((steps,)),
            pltpu.SemaphoreType.DMA((steps,)),
            pltpu.SemaphoreType.DMA((2,)),
            pltpu.SemaphoreType.DMA((steps * inner,)),
            pltpu.SemaphoreType.DMA((steps * inner,)),
            pltpu.SemaphoreType.DMA((steps,)),
        ],
        cost_estimate=pl.CostEstimate(flops=0, bytes_accessed=sent * 4, transcendentals=0),
        compiler_params=pltpu.CompilerParams(
            collective_id=branch, has_side_effects=True, vmem_limit_bytes=60 * 1024 * 1024
        ),
    )(positions, master_send, update_send)


def shards(master, first_moment, second_moment, rotation, assignment):
    dp_count = lax.axis_size("dp")
    group_count = lax.axis_size("expert")
    position = lax.axis_index("dp")
    group_id = lax.axis_index("expert")
    round_count = rotation.shape[0]
    rows_here = master.shape[1]
    lane_count = LANE
    per_row = master.shape[2] // lane_count
    lines_device = rows_here * per_row
    piece_len = lines_device // (round_count * dp_count)
    inv_count = 1.0 / math.sqrt(dp_count * piece_len * lane_count)
    table = slot_table(rotation, dp_count, MOST)
    span_count = round_count * dp_count
    inner = INNER
    planes = dp_count // inner
    slots = round_count * MOST

    plane_of = rotation.reshape(span_count) // inner
    span_ids = jnp.arange(span_count, dtype=jnp.int32)
    same = (plane_of[:, None] == plane_of[None, :]) & (span_ids[None, :] < span_ids[:, None])
    place_of = jnp.sum(same.astype(jnp.int32), axis=1)
    plane_ids = jnp.arange(planes, dtype=jnp.int32)
    loads = jnp.sum((plane_of[None, :] == plane_ids[:, None]).astype(jnp.int32), axis=1)
    most_load = jnp.max(loads)
    cap_all = min(inner * slots, span_count)
    mean_load = span_count // planes
    caps = sorted({min(cap_all, mean_load * 3 // 2), min(cap_all, mean_load * 2), cap_all})
    choice = sum((most_load > cap).astype(jnp.int32) for cap in caps[:-1])
    place_ids = jnp.arange(cap_all, dtype=jnp.int32)
    listed = (plane_of[None, None, :] == plane_ids[:, None, None]) & (
        place_of[None, None, :] == place_ids[None, :, None]
    )
    lists = jnp.sum(listed.astype(jnp.int32) * span_ids, axis=2)
    mine = table.transpose(2, 0, 1).reshape(planes, inner, round_count, MOST)
    mine = lax.dynamic_index_in_dim(mine, position // inner, 0, keepdims=False)
    padded_place = jnp.concatenate(
        [place_of.reshape(round_count, dp_count), jnp.full((round_count, 1), cap_all, jnp.int32)], axis=1
    )
    hits = mine[..., None] == jnp.arange(dp_count + 1, dtype=jnp.int32)
    positions = jnp.sum(hits * padded_place[None, :, None, :], axis=3).reshape(inner, slots)

    update = scaled_moment(first_moment, second_moment)
    master_lines = master.reshape(span_count, piece_len, lane_count)
    update_lines = update.reshape(span_count, piece_len, lane_count)
    local_lines = position * lines_device + jnp.arange(lines_device, dtype=jnp.int32).reshape(
        span_count, piece_len
    )
    weights = position_weights(local_lines, per_row, lane_count)
    master_sums = jnp.sum(master_lines * weights, axis=(1, 2)) * inv_count
    update_sums = jnp.sum(update_lines * weights, axis=(1, 2)) * inv_count

    def branch_of(number, cap):
        def run(master_in, update_in):
            chosen = lists[:, :cap]
            return exchange(
                planes, inner, slots, cap, number, positions, master_in[chosen], update_in[chosen]
            )

        return run

    saved_master, saved_update = lax.switch(
        choice, [branch_of(number, cap) for number, cap in enumerate(caps)], master_lines, update_lines
    )
    slot_ids = jnp.arange(span_count, dtype=jnp.int32)
    permuting = (assignment[:, None] == slot_ids[None, :]).astype(jnp.float32)
    both_sums = jnp.stack([master_sums, update_sums])
    placed_sums = jnp.sum(both_sums[:, :, None] * permuting[None], axis=1)
    in_slot = (jnp.arange(group_count, dtype=jnp.int32) == group_id).astype(jnp.float32)
    contribution = in_slot[:, None, None] * placed_sums[None]
    checksums = lax.psum(contribution, ("dp", "expert"))
    shape_out = (1, round_count, MOST, dp_count * piece_len, lane_count)
    return (saved_master.reshape(shape_out), saved_update.reshape(shape_out), checksums)


def solution(mesh):
    placed = (P("expert", "dp", None), P("expert", "dp", None), P("expert", "dp", None), P(), P())
    return jax.shard_map(
        shards,
        mesh=mesh,
        in_specs=placed,
        out_specs=(P("expert", "dp", None, None, None), P("expert", "dp", None, None, None), P()),
        check_vma=False,
    )
```

```python
import functools
import math

import jax
import jax.numpy as jnp
from jax import lax
from jax.experimental import pallas as pl
from jax.experimental.pallas import tpu as pltpu
from jax.sharding import PartitionSpec as P

LANE = 128
MOST = 3
STEP = 20
INNER = 4


BETA_ONE = 0.9
BETA_TWO = 0.95
EPSILON = 1e-08


def scaled_moment(first_part, second_part):
    corr_one = 1.0 - BETA_ONE**STEP
    corr_two = 1.0 - BETA_TWO**STEP
    return first_part / corr_one / (jnp.sqrt(second_part / corr_two) + EPSILON)


def slot_table(rotation, dp_count, most_slots):
    owners = rotation[:, :, 0]
    span_ids = jnp.arange(dp_count, dtype=jnp.int32)
    same_writer = owners[:, :, None] == owners[:, None, :]
    before = span_ids[None, :] < span_ids[:, None]
    slot_rank = jnp.sum((same_writer & before[None]).astype(jnp.int32), axis=2)
    writers = jnp.arange(dp_count, dtype=jnp.int32)
    slot_ids = jnp.arange(most_slots, dtype=jnp.int32)
    matches = (owners[:, None, None, :] == writers[None, None, :, None]) & (
        slot_rank[:, None, None, :] == slot_ids[None, :, None, None]
    )
    matches = matches.astype(jnp.int32)
    found_any = jnp.sum(matches, axis=3)
    picked = jnp.sum(matches * span_ids, axis=3)
    return picked + (1 - found_any) * dp_count


def position_weights(line_ids, per_row, lane_count):
    row_ids = line_ids // per_row
    col_ids = line_ids % per_row * lane_count
    lane_ids = jnp.arange(lane_count, dtype=jnp.int32)
    pattern = (row_ids[..., None] * 5 + (col_ids[..., None] + lane_ids) * 3) % 11
    return 1.0 + pattern.astype(jnp.float32) / 10.0


def exchange_kernel(
    planes, inner, groups, slots, cap, pos_ref, sum_ref, m_ref, u_ref, om_ref, ou_ref, oc_ref, *scratch
):
    held = scratch[: 2 * planes]
    stage = scratch[2 * planes : 4 * planes]
    zs_sem, zr_sem, local_sem, is_sem, ir_sem, self_sem = scratch[4 * planes : 4 * planes + 6]
    by_plane, by_spot, by_group, cs_sem, cr_sem, cl_sem = scratch[4 * planes + 6 :]
    me = lax.axis_index("dp")
    plane = me // inner
    spot = me % inner
    core = lax.axis_index("expert")
    fields = (m_ref, u_ref)
    outs = (om_ref, ou_ref)

    def peer(plane_to, spot_to):
        return (plane_to * inner + spot_to, core)

    barrier = pltpu.get_barrier_semaphore()
    for d in range(1, planes):
        pl.semaphore_signal(
            barrier, inc=1, device_id=peer((plane + d) % planes, spot), device_id_type=pl.DeviceIdType.MESH
        )
    for e in range(1, inner):
        pl.semaphore_signal(
            barrier, inc=1, device_id=peer(plane, (spot + e) % inner), device_id_type=pl.DeviceIdType.MESH
        )
    for g in range(1, groups):
        pl.semaphore_signal(
            barrier, inc=1, device_id=(me, (core + g) % groups), device_id_type=pl.DeviceIdType.MESH
        )
    pl.semaphore_wait(barrier, planes + inner + groups - 3)

    def small(src, dst, number, to):
        copy = pltpu.make_async_remote_copy(
            src_ref=src,
            dst_ref=dst,
            send_sem=cs_sem.at[number],
            recv_sem=cr_sem.at[number],
            device_id=to,
            device_id_type=pl.DeviceIdType.MESH,
        )
        copy.start()
        return copy

    own_sums = pltpu.make_async_copy(sum_ref, by_plane.at[0], cl_sem.at[0])
    own_sums.start()
    sums_far = [
        small(sum_ref, by_plane.at[d], d, peer((plane + d) % planes, spot)) for d in range(1, planes)
    ]

    far = [None] * (2 * planes)
    for f in range(2):
        own = pltpu.make_async_copy(fields[f].at[plane], held[f * planes], local_sem.at[f])
        own.start()
        far[f * planes] = own
        for d in range(1, planes):
            to_plane = (plane + d) % planes
            copy = pltpu.make_async_remote_copy(
                src_ref=fields[f].at[to_plane],
                dst_ref=held[f * planes + d],
                send_sem=zs_sem.at[f * planes + d],
                recv_sem=zr_sem.at[f * planes + d],
                device_id=peer(to_plane, spot),
                device_id_type=pl.DeviceIdType.MESH,
            )
            copy.start()
            far[f * planes + d] = copy

    own_sums.wait()
    for copy in sums_far:
        copy.wait()
    kept_sums = pltpu.make_async_copy(by_plane, by_spot.at[0], cl_sem.at[1])
    kept_sums.start()
    sums_near = [
        small(by_plane, by_spot.at[e], planes + e, peer(plane, (spot + e) % inner)) for e in range(1, inner)
    ]

    near = []
    for f in range(2):
        for d in range(planes):
            g = f * planes + d
            if d == 0:
                far[g].wait()
            else:
                far[g].wait_recv()

            def place(t, carry, g=g):
                e = t // slots
                s = t % slots
                index = pos_ref[(spot + e) % inner, s]
                found = index < cap
                lines = held[g][jnp.where(found, index, 0)]
                stage[g][e, s] = jnp.where(found, lines, 0.0)
                return carry

            lax.fori_loop(0, inner * slots, place, 0)
            source = ((plane + planes - d) % planes) * inner + spot
            for e in range(1, inner):
                copy = pltpu.make_async_remote_copy(
                    src_ref=stage[g].at[e],
                    dst_ref=outs[f].at[:, source],
                    send_sem=is_sem.at[g * inner + e],
                    recv_sem=ir_sem.at[g * inner + e],
                    device_id=peer(plane, (spot + e) % inner),
                    device_id_type=pl.DeviceIdType.MESH,
                )
                copy.start()
                near.append(copy)
            copy = pltpu.make_async_copy(stage[g].at[0], outs[f].at[:, source], self_sem.at[g])
            copy.start()
            near.append(copy)
    kept_sums.wait()
    for copy in sums_near:
        copy.wait()
    sums_across = [
        small(by_spot, by_group.at[g], planes + inner + g, (me, (core + g) % groups))
        for g in range(1, groups)
    ]
    oc_ref[core] = jnp.sum(by_spot[...], axis=(0, 1))
    for g in range(1, groups):
        sums_across[g - 1].wait()
        oc_ref[(core + groups - g) % groups] = jnp.sum(by_group[g], axis=(0, 1))
    for f in range(2):
        for d in range(1, planes):
            far[f * planes + d].wait_send()
    for copy in near:
        copy.wait()


def exchange(planes, inner, groups, slots, cap, branch, positions, sums, master_send, update_send):
    lines, lanes = master_send.shape[2:]
    shape = jax.ShapeDtypeStruct((slots, planes * inner, lines, lanes), jnp.float32)
    any_space = pl.BlockSpec(memory_space=pl.ANY)
    steps = 2 * planes
    tile = sums.shape
    hops = planes + inner + groups
    sent = (planes - 1) * cap * 2 * lines * lanes * 4
    return pl.pallas_call(
        functools.partial(exchange_kernel, planes, inner, groups, slots, cap),
        out_shape=(shape, shape, jax.ShapeDtypeStruct((groups, *tile), jnp.float32)),
        in_specs=[
            pl.BlockSpec(memory_space=pltpu.SMEM),
            pl.BlockSpec(memory_space=pltpu.VMEM),
            any_space,
            any_space,
        ],
        out_specs=(any_space, any_space, pl.BlockSpec(memory_space=pltpu.VMEM)),
        scratch_shapes=[pltpu.VMEM((cap, lines, lanes), jnp.float32)] * steps
        + [pltpu.VMEM((inner, slots, lines, lanes), jnp.float32)] * steps
        + [
            pltpu.SemaphoreType.DMA((steps,)),
            pltpu.SemaphoreType.DMA((steps,)),
            pltpu.SemaphoreType.DMA((2,)),
            pltpu.SemaphoreType.DMA((steps * inner,)),
            pltpu.SemaphoreType.DMA((steps * inner,)),
            pltpu.SemaphoreType.DMA((steps,)),
            pltpu.VMEM((planes, *tile), jnp.float32),
            pltpu.VMEM((inner, planes, *tile), jnp.float32),
            pltpu.VMEM((groups, inner, planes, *tile), jnp.float32),
            pltpu.SemaphoreType.DMA((hops,)),
            pltpu.SemaphoreType.DMA((hops,)),
            pltpu.SemaphoreType.DMA((2,)),
        ],
        cost_estimate=pl.CostEstimate(flops=0, bytes_accessed=sent * 4, transcendentals=0),
        compiler_params=pltpu.CompilerParams(
            collective_id=branch, has_side_effects=True, vmem_limit_bytes=60 * 1024 * 1024
        ),
    )(positions, sums, master_send, update_send)


def shards(master, first_moment, second_moment, rotation, assignment):
    dp_count = lax.axis_size("dp")
    group_count = lax.axis_size("expert")
    position = lax.axis_index("dp")
    round_count = rotation.shape[0]
    rows_here = master.shape[1]
    lane_count = LANE
    per_row = master.shape[2] // lane_count
    lines_device = rows_here * per_row
    piece_len = lines_device // (round_count * dp_count)
    inv_count = 1.0 / math.sqrt(dp_count * piece_len * lane_count)
    table = slot_table(rotation, dp_count, MOST)
    span_count = round_count * dp_count
    inner = INNER
    planes = dp_count // inner
    slots = round_count * MOST

    plane_of = rotation.reshape(span_count) // inner
    span_ids = jnp.arange(span_count, dtype=jnp.int32)
    same = (plane_of[:, None] == plane_of[None, :]) & (span_ids[None, :] < span_ids[:, None])
    place_of = jnp.sum(same.astype(jnp.int32), axis=1)
    plane_ids = jnp.arange(planes, dtype=jnp.int32)
    loads = jnp.sum((plane_of[None, :] == plane_ids[:, None]).astype(jnp.int32), axis=1)
    most_load = jnp.max(loads)
    cap_all = min(inner * slots, span_count)
    mean_load = span_count // planes
    caps = sorted({min(cap_all, mean_load * 3 // 2), min(cap_all, mean_load * 2), cap_all})
    choice = sum((most_load > cap).astype(jnp.int32) for cap in caps[:-1])
    place_ids = jnp.arange(cap_all, dtype=jnp.int32)
    listed = (plane_of[None, None, :] == plane_ids[:, None, None]) & (
        place_of[None, None, :] == place_ids[None, :, None]
    )
    lists = jnp.sum(listed.astype(jnp.int32) * span_ids, axis=2)
    mine = table.transpose(2, 0, 1).reshape(planes, inner, round_count, MOST)
    mine = lax.dynamic_index_in_dim(mine, position // inner, 0, keepdims=False)
    padded_place = jnp.concatenate(
        [place_of.reshape(round_count, dp_count), jnp.full((round_count, 1), cap_all, jnp.int32)], axis=1
    )
    hits = mine[..., None] == jnp.arange(dp_count + 1, dtype=jnp.int32)
    positions = jnp.sum(hits * padded_place[None, :, None, :], axis=3).reshape(inner, slots)

    update = scaled_moment(first_moment, second_moment)
    master_lines = master.reshape(span_count, piece_len, lane_count)
    update_lines = update.reshape(span_count, piece_len, lane_count)
    local_lines = position * lines_device + jnp.arange(lines_device, dtype=jnp.int32).reshape(
        span_count, piece_len
    )
    weights = position_weights(local_lines, per_row, lane_count)
    master_sums = jnp.sum(master_lines * weights, axis=(1, 2)) * inv_count
    update_sums = jnp.sum(update_lines * weights, axis=(1, 2)) * inv_count

    permuting = (assignment[:, None] == span_ids[None, :]).astype(jnp.float32)
    both_sums = jnp.stack([master_sums, update_sums])
    placed_sums = jnp.sum(both_sums[:, :, None] * permuting[None], axis=1)
    entries = 2 * span_count
    tile_size = 8 * lane_count
    sums = jnp.pad(placed_sums.reshape(entries), (0, -entries % tile_size)).reshape(-1, lane_count)

    def branch_of(number, cap):
        def run(master_in, update_in):
            chosen = lists[:, :cap]
            return exchange(
                planes,
                inner,
                group_count,
                slots,
                cap,
                number,
                positions,
                sums,
                master_in[chosen],
                update_in[chosen],
            )

        return run

    saved_master, saved_update, totals = lax.switch(
        choice, [branch_of(number, cap) for number, cap in enumerate(caps)], master_lines, update_lines
    )
    checksums = totals.reshape(group_count, -1)[:, :entries].reshape(group_count, 2, span_count)
    shape_out = (1, round_count, MOST, dp_count * piece_len, lane_count)
    return (saved_master.reshape(shape_out), saved_update.reshape(shape_out), checksums)


def solution(mesh):
    placed = (P("expert", "dp", None), P("expert", "dp", None), P("expert", "dp", None), P(), P())
    return jax.shard_map(
        shards,
        mesh=mesh,
        in_specs=placed,
        out_specs=(P("expert", "dp", None, None, None), P("expert", "dp", None, None, None), P()),
        check_vma=False,
    )
```

```python
import functools
import math

import jax
import jax.numpy as jnp
from jax import lax
from jax.experimental import pallas as pl
from jax.experimental.pallas import tpu as pltpu
from jax.sharding import PartitionSpec as P

LANE = 128
MOST = 3
STEP = 20
INNER = 4


BETA_ONE = 0.9
BETA_TWO = 0.95
EPSILON = 1e-08


def scaled_moment(first_part, second_part):
    corr_one = 1.0 - BETA_ONE**STEP
    corr_two = 1.0 - BETA_TWO**STEP
    return first_part / corr_one / (jnp.sqrt(second_part / corr_two) + EPSILON)


def slot_table(rotation, dp_count, most_slots):
    owners = rotation[:, :, 0]
    span_ids = jnp.arange(dp_count, dtype=jnp.int32)
    same_writer = owners[:, :, None] == owners[:, None, :]
    before = span_ids[None, :] < span_ids[:, None]
    slot_rank = jnp.sum((same_writer & before[None]).astype(jnp.int32), axis=2)
    writers = jnp.arange(dp_count, dtype=jnp.int32)
    slot_ids = jnp.arange(most_slots, dtype=jnp.int32)
    matches = (owners[:, None, None, :] == writers[None, None, :, None]) & (
        slot_rank[:, None, None, :] == slot_ids[None, :, None, None]
    )
    matches = matches.astype(jnp.int32)
    found_any = jnp.sum(matches, axis=3)
    picked = jnp.sum(matches * span_ids, axis=3)
    return picked + (1 - found_any) * dp_count


def position_weights(line_ids, per_row, lane_count):
    row_ids = line_ids // per_row
    col_ids = line_ids % per_row * lane_count
    lane_ids = jnp.arange(lane_count, dtype=jnp.int32)
    pattern = (row_ids[..., None] * 5 + (col_ids[..., None] + lane_ids) * 3) % 11
    return 1.0 + pattern.astype(jnp.float32) / 10.0


def exchange_kernel(
    planes, inner, groups, slots, cap, pos_ref, sum_ref, m_ref, u_ref, om_ref, ou_ref, oc_ref, *scratch
):
    held = scratch[: 2 * planes]
    stage = scratch[2 * planes : 4 * planes]
    zs_sem, zr_sem, local_sem, is_sem, ir_sem, self_sem = scratch[4 * planes : 4 * planes + 6]
    by_plane, by_spot, by_group, cs_sem, cr_sem, cl_sem = scratch[4 * planes + 6 :]
    me = lax.axis_index("dp")
    plane = me // inner
    spot = me % inner
    core = lax.axis_index("expert")
    fields = (m_ref, u_ref)
    outs = (om_ref, ou_ref)

    def peer(plane_to, spot_to):
        return (plane_to * inner + spot_to, core)

    barrier = pltpu.get_barrier_semaphore()
    for d in range(1, planes):
        pl.semaphore_signal(
            barrier, inc=1, device_id=peer((plane + d) % planes, spot), device_id_type=pl.DeviceIdType.MESH
        )
    for e in range(1, inner):
        pl.semaphore_signal(
            barrier, inc=1, device_id=peer(plane, (spot + e) % inner), device_id_type=pl.DeviceIdType.MESH
        )
    for g in range(1, groups):
        pl.semaphore_signal(
            barrier, inc=1, device_id=(me, (core + g) % groups), device_id_type=pl.DeviceIdType.MESH
        )
    pl.semaphore_wait(barrier, planes + inner + groups - 3)

    def small(src, dst, number, to):
        copy = pltpu.make_async_remote_copy(
            src_ref=src,
            dst_ref=dst,
            send_sem=cs_sem.at[number],
            recv_sem=cr_sem.at[number],
            device_id=to,
            device_id_type=pl.DeviceIdType.MESH,
        )
        copy.start()
        return copy

    own_sums = pltpu.make_async_copy(sum_ref, by_plane.at[0], cl_sem.at[0])
    own_sums.start()
    sums_far = [
        small(sum_ref, by_plane.at[d], d, peer((plane + d) % planes, spot)) for d in range(1, planes)
    ]

    far = [None] * (2 * planes)
    for f in range(2):
        own = pltpu.make_async_copy(fields[f].at[plane], held[f * planes], local_sem.at[f])
        own.start()
        far[f * planes] = own
        for d in range(1, planes):
            to_plane = (plane + d) % planes
            copy = pltpu.make_async_remote_copy(
                src_ref=fields[f].at[to_plane],
                dst_ref=held[f * planes + d],
                send_sem=zs_sem.at[f * planes + d],
                recv_sem=zr_sem.at[f * planes + d],
                device_id=peer(to_plane, spot),
                device_id_type=pl.DeviceIdType.MESH,
            )
            copy.start()
            far[f * planes + d] = copy

    own_sums.wait()
    for copy in sums_far:
        copy.wait()
    kept_sums = pltpu.make_async_copy(by_plane, by_spot.at[0], cl_sem.at[1])
    kept_sums.start()
    sums_near = [
        small(by_plane, by_spot.at[e], planes + e, peer(plane, (spot + e) % inner)) for e in range(1, inner)
    ]

    near = []
    for f in range(2):
        for d in range(planes):
            g = f * planes + d
            if d == 0:
                far[g].wait()
            else:
                far[g].wait_recv()

            def place(t, carry, g=g):
                e = t // slots
                s = t % slots
                index = pos_ref[(spot + e) % inner, s]
                found = index < cap
                lines = held[g][jnp.where(found, index, 0)]
                stage[g][e, s] = jnp.where(found, lines, 0.0)
                return carry

            lax.fori_loop(0, inner * slots, place, 0)
            source = ((plane + planes - d) % planes) * inner + spot
            for e in range(1, inner):
                copy = pltpu.make_async_remote_copy(
                    src_ref=stage[g].at[e],
                    dst_ref=outs[f].at[:, source],
                    send_sem=is_sem.at[g * inner + e],
                    recv_sem=ir_sem.at[g * inner + e],
                    device_id=peer(plane, (spot + e) % inner),
                    device_id_type=pl.DeviceIdType.MESH,
                )
                copy.start()
                near.append(copy)
            copy = pltpu.make_async_copy(stage[g].at[0], outs[f].at[:, source], self_sem.at[g])
            copy.start()
            near.append(copy)
    kept_sums.wait()
    for copy in sums_near:
        copy.wait()
    sums_across = [
        small(by_spot, by_group.at[g], planes + inner + g, (me, (core + g) % groups))
        for g in range(1, groups)
    ]
    oc_ref[core] = jnp.sum(by_spot[...], axis=(0, 1))
    for g in range(1, groups):
        sums_across[g - 1].wait()
        oc_ref[(core + groups - g) % groups] = jnp.sum(by_group[g], axis=(0, 1))
    for f in range(2):
        for d in range(1, planes):
            far[f * planes + d].wait_send()
    for copy in near:
        copy.wait()


def exchange(planes, inner, groups, slots, cap, branch, positions, sums, master_send, update_send):
    lines, lanes = master_send.shape[2:]
    shape = jax.ShapeDtypeStruct((slots, planes * inner, lines, lanes), jnp.float32)
    any_space = pl.BlockSpec(memory_space=pl.ANY)
    steps = 2 * planes
    tile = sums.shape
    hops = planes + inner + groups
    sent = (planes - 1) * cap * 2 * lines * lanes * 4
    return pl.pallas_call(
        functools.partial(exchange_kernel, planes, inner, groups, slots, cap),
        out_shape=(shape, shape, jax.ShapeDtypeStruct((groups, *tile), jnp.float32)),
        in_specs=[
            pl.BlockSpec(memory_space=pltpu.SMEM),
            pl.BlockSpec(memory_space=pltpu.VMEM),
            any_space,
            any_space,
        ],
        out_specs=(any_space, any_space, pl.BlockSpec(memory_space=pltpu.VMEM)),
        scratch_shapes=[pltpu.VMEM((cap, lines, lanes), jnp.float32)] * steps
        + [pltpu.VMEM((inner, slots, lines, lanes), jnp.float32)] * steps
        + [
            pltpu.SemaphoreType.DMA((steps,)),
            pltpu.SemaphoreType.DMA((steps,)),
            pltpu.SemaphoreType.DMA((2,)),
            pltpu.SemaphoreType.DMA((steps * inner,)),
            pltpu.SemaphoreType.DMA((steps * inner,)),
            pltpu.SemaphoreType.DMA((steps,)),
            pltpu.VMEM((planes, *tile), jnp.float32),
            pltpu.VMEM((inner, planes, *tile), jnp.float32),
            pltpu.VMEM((groups, inner, planes, *tile), jnp.float32),
            pltpu.SemaphoreType.DMA((hops,)),
            pltpu.SemaphoreType.DMA((hops,)),
            pltpu.SemaphoreType.DMA((2,)),
        ],
        cost_estimate=pl.CostEstimate(flops=0, bytes_accessed=sent * 4, transcendentals=0),
        compiler_params=pltpu.CompilerParams(
            collective_id=branch, has_side_effects=True, vmem_limit_bytes=60 * 1024 * 1024
        ),
    )(positions, sums, master_send, update_send)


def shards(master, first_moment, second_moment, rotation, assignment):
    dp_count = lax.axis_size("dp")
    group_count = lax.axis_size("expert")
    position = lax.axis_index("dp")
    round_count = rotation.shape[0]
    rows_here = master.shape[1]
    lane_count = LANE
    per_row = master.shape[2] // lane_count
    lines_device = rows_here * per_row
    piece_len = lines_device // (round_count * dp_count)
    inv_count = 1.0 / math.sqrt(dp_count * piece_len * lane_count)
    table = slot_table(rotation, dp_count, MOST)
    span_count = round_count * dp_count
    inner = INNER
    planes = dp_count // inner
    slots = round_count * MOST

    plane_of = rotation.reshape(span_count) // inner
    span_ids = jnp.arange(span_count, dtype=jnp.int32)
    same = (plane_of[:, None] == plane_of[None, :]) & (span_ids[None, :] < span_ids[:, None])
    place_of = jnp.sum(same.astype(jnp.int32), axis=1)
    plane_ids = jnp.arange(planes, dtype=jnp.int32)
    loads = jnp.sum((plane_of[None, :] == plane_ids[:, None]).astype(jnp.int32), axis=1)
    most_load = jnp.max(loads)
    cap_all = min(inner * slots, span_count)
    mean_load = span_count // planes
    caps = sorted({min(cap_all, mean_load * eighths // 8) for eighths in (10, 11, 12, 13, 14, 16)} | {cap_all})
    choice = sum((most_load > cap).astype(jnp.int32) for cap in caps[:-1])
    place_ids = jnp.arange(cap_all, dtype=jnp.int32)
    listed = (plane_of[None, None, :] == plane_ids[:, None, None]) & (
        place_of[None, None, :] == place_ids[None, :, None]
    )
    lists = jnp.sum(listed.astype(jnp.int32) * span_ids, axis=2)
    mine = table.transpose(2, 0, 1).reshape(planes, inner, round_count, MOST)
    mine = lax.dynamic_index_in_dim(mine, position // inner, 0, keepdims=False)
    padded_place = jnp.concatenate(
        [place_of.reshape(round_count, dp_count), jnp.full((round_count, 1), cap_all, jnp.int32)], axis=1
    )
    hits = mine[..., None] == jnp.arange(dp_count + 1, dtype=jnp.int32)
    positions = jnp.sum(hits * padded_place[None, :, None, :], axis=3).reshape(inner, slots)

    update = scaled_moment(first_moment, second_moment)
    master_lines = master.reshape(span_count, piece_len, lane_count)
    update_lines = update.reshape(span_count, piece_len, lane_count)
    local_lines = position * lines_device + jnp.arange(lines_device, dtype=jnp.int32).reshape(
        span_count, piece_len
    )
    weights = position_weights(local_lines, per_row, lane_count)
    master_sums = jnp.sum(master_lines * weights, axis=(1, 2)) * inv_count
    update_sums = jnp.sum(update_lines * weights, axis=(1, 2)) * inv_count

    permuting = (assignment[:, None] == span_ids[None, :]).astype(jnp.float32)
    both_sums = jnp.stack([master_sums, update_sums])
    placed_sums = jnp.sum(both_sums[:, :, None] * permuting[None], axis=1)
    entries = 2 * span_count
    tile_size = 8 * lane_count
    sums = jnp.pad(placed_sums.reshape(entries), (0, -entries % tile_size)).reshape(-1, lane_count)

    def branch_of(number, cap):
        def run(master_in, update_in):
            chosen = lists[:, :cap]
            return exchange(
                planes,
                inner,
                group_count,
                slots,
                cap,
                number,
                positions,
                sums,
                master_in[chosen],
                update_in[chosen],
            )

        return run

    saved_master, saved_update, totals = lax.switch(
        choice, [branch_of(number, cap) for number, cap in enumerate(caps)], master_lines, update_lines
    )
    checksums = totals.reshape(group_count, -1)[:, :entries].reshape(group_count, 2, span_count)
    shape_out = (1, round_count, MOST, dp_count * piece_len, lane_count)
    return (saved_master.reshape(shape_out), saved_update.reshape(shape_out), checksums)


def solution(mesh):
    placed = (P("expert", "dp", None), P("expert", "dp", None), P("expert", "dp", None), P(), P())
    return jax.shard_map(
        shards,
        mesh=mesh,
        in_specs=placed,
        out_specs=(P("expert", "dp", None, None, None), P("expert", "dp", None, None, None), P()),
        check_vma=False,
    )
```

```python
import functools
import math

import jax
import jax.numpy as jnp
from jax import lax
from jax.experimental import pallas as pl
from jax.experimental.pallas import tpu as pltpu
from jax.sharding import PartitionSpec as P

LANE = 128
MOST = 3
STEP = 20
INNER = 4


BETA_ONE = 0.9
BETA_TWO = 0.95
EPSILON = 1e-08


def scaled_moment(first_part, second_part):
    corr_one = 1.0 - BETA_ONE**STEP
    corr_two = 1.0 - BETA_TWO**STEP
    return first_part / corr_one / (jnp.sqrt(second_part / corr_two) + EPSILON)


def slot_table(rotation, dp_count, most_slots):
    owners = rotation[:, :, 0]
    span_ids = jnp.arange(dp_count, dtype=jnp.int32)
    same_writer = owners[:, :, None] == owners[:, None, :]
    before = span_ids[None, :] < span_ids[:, None]
    slot_rank = jnp.sum((same_writer & before[None]).astype(jnp.int32), axis=2)
    writers = jnp.arange(dp_count, dtype=jnp.int32)
    slot_ids = jnp.arange(most_slots, dtype=jnp.int32)
    matches = (owners[:, None, None, :] == writers[None, None, :, None]) & (
        slot_rank[:, None, None, :] == slot_ids[None, :, None, None]
    )
    matches = matches.astype(jnp.int32)
    found_any = jnp.sum(matches, axis=3)
    picked = jnp.sum(matches * span_ids, axis=3)
    return picked + (1 - found_any) * dp_count


def position_weights(line_ids, per_row, lane_count):
    row_ids = line_ids // per_row
    col_ids = line_ids % per_row * lane_count
    lane_ids = jnp.arange(lane_count, dtype=jnp.int32)
    pattern = (row_ids[..., None] * 5 + (col_ids[..., None] + lane_ids) * 3) % 11
    return 1.0 + pattern.astype(jnp.float32) / 10.0


def exchange_kernel(
    planes, inner, groups, slots, cap, pos_ref, sum_ref, m_ref, u_ref, om_ref, ou_ref, oc_ref, *scratch
):
    held = scratch[: 2 * planes]
    stage = scratch[2 * planes : 4 * planes]
    zs_sem, zr_sem, local_sem, is_sem, ir_sem, self_sem = scratch[4 * planes : 4 * planes + 6]
    by_plane, by_spot, by_group, cs_sem, cr_sem, cl_sem = scratch[4 * planes + 6 :]
    me = lax.axis_index("dp")
    plane = me // inner
    spot = me % inner
    core = lax.axis_index("expert")
    fields = (m_ref, u_ref)
    outs = (om_ref, ou_ref)

    def peer(plane_to, spot_to):
        return (plane_to * inner + spot_to, core)

    def mate(d):
        other, bit = plane, 1
        while bit < planes:
            if d & bit:
                other = other + bit * (1 - 2 * ((plane // bit) % 2))
            bit *= 2
        return other

    barrier = pltpu.get_barrier_semaphore()
    for d in range(1, planes):
        pl.semaphore_signal(
            barrier, inc=1, device_id=peer(mate(d), spot), device_id_type=pl.DeviceIdType.MESH
        )
    for e in range(1, inner):
        pl.semaphore_signal(
            barrier, inc=1, device_id=peer(plane, (spot + e) % inner), device_id_type=pl.DeviceIdType.MESH
        )
    for g in range(1, groups):
        pl.semaphore_signal(
            barrier, inc=1, device_id=(me, (core + g) % groups), device_id_type=pl.DeviceIdType.MESH
        )
    pl.semaphore_wait(barrier, planes + inner + groups - 3)

    def small(src, dst, number, to):
        copy = pltpu.make_async_remote_copy(
            src_ref=src,
            dst_ref=dst,
            send_sem=cs_sem.at[number],
            recv_sem=cr_sem.at[number],
            device_id=to,
            device_id_type=pl.DeviceIdType.MESH,
        )
        copy.start()
        return copy

    own_sums = pltpu.make_async_copy(sum_ref, by_plane.at[0], cl_sem.at[0])
    own_sums.start()
    sums_far = [
        small(sum_ref, by_plane.at[d], d, peer(mate(d), spot)) for d in range(1, planes)
    ]

    far = [None] * (2 * planes)
    for f in range(2):
        own = pltpu.make_async_copy(fields[f].at[plane], held[f * planes], local_sem.at[f])
        own.start()
        far[f * planes] = own
        for d in range(1, planes):
            to_plane = mate(d)
            copy = pltpu.make_async_remote_copy(
                src_ref=fields[f].at[to_plane],
                dst_ref=held[f * planes + d],
                send_sem=zs_sem.at[f * planes + d],
                recv_sem=zr_sem.at[f * planes + d],
                device_id=peer(to_plane, spot),
                device_id_type=pl.DeviceIdType.MESH,
            )
            copy.start()
            far[f * planes + d] = copy

    own_sums.wait()
    for copy in sums_far:
        copy.wait()
    kept_sums = pltpu.make_async_copy(by_plane, by_spot.at[0], cl_sem.at[1])
    kept_sums.start()
    sums_near = [
        small(by_plane, by_spot.at[e], planes + e, peer(plane, (spot + e) % inner)) for e in range(1, inner)
    ]

    near = []
    order = [(f, 0) for f in range(2)] + [(f, d) for f in range(2) for d in range(1, planes)]
    for f, d in order:
        g = f * planes + d
        if d == 0:
            far[g].wait()
        else:
            far[g].wait_recv()

        def place(t, carry, g=g):
            e = t // slots
            s = t % slots
            index = pos_ref[(spot + e) % inner, s]
            found = index < cap
            lines = held[g][jnp.where(found, index, 0)]
            stage[g][e, s] = jnp.where(found, lines, 0.0)
            return carry

        lax.fori_loop(0, inner * slots, place, 0)
        source = mate(d) * inner + spot
        for e in range(1, inner):
            copy = pltpu.make_async_remote_copy(
                src_ref=stage[g].at[e],
                dst_ref=outs[f].at[:, source],
                send_sem=is_sem.at[g * inner + e],
                recv_sem=ir_sem.at[g * inner + e],
                device_id=peer(plane, (spot + e) % inner),
                device_id_type=pl.DeviceIdType.MESH,
            )
            copy.start()
            near.append(copy)
        copy = pltpu.make_async_copy(stage[g].at[0], outs[f].at[:, source], self_sem.at[g])
        copy.start()
        near.append(copy)
    kept_sums.wait()
    for copy in sums_near:
        copy.wait()
    sums_across = [
        small(by_spot, by_group.at[g], planes + inner + g, (me, (core + g) % groups))
        for g in range(1, groups)
    ]
    oc_ref[core] = jnp.sum(by_spot[...], axis=(0, 1))
    for g in range(1, groups):
        sums_across[g - 1].wait()
        oc_ref[(core + groups - g) % groups] = jnp.sum(by_group[g], axis=(0, 1))
    for f in range(2):
        for d in range(1, planes):
            far[f * planes + d].wait_send()
    for copy in near:
        copy.wait()


def exchange(planes, inner, groups, slots, cap, branch, positions, sums, master_send, update_send):
    lines, lanes = master_send.shape[2:]
    shape = jax.ShapeDtypeStruct((slots, planes * inner, lines, lanes), jnp.float32)
    any_space = pl.BlockSpec(memory_space=pl.ANY)
    steps = 2 * planes
    tile = sums.shape
    hops = planes + inner + groups
    sent = (planes - 1) * cap * 2 * lines * lanes * 4
    return pl.pallas_call(
        functools.partial(exchange_kernel, planes, inner, groups, slots, cap),
        out_shape=(shape, shape, jax.ShapeDtypeStruct((groups, *tile), jnp.float32)),
        in_specs=[
            pl.BlockSpec(memory_space=pltpu.SMEM),
            pl.BlockSpec(memory_space=pltpu.VMEM),
            any_space,
            any_space,
        ],
        out_specs=(any_space, any_space, pl.BlockSpec(memory_space=pltpu.VMEM)),
        scratch_shapes=[pltpu.VMEM((cap, lines, lanes), jnp.float32)] * steps
        + [pltpu.VMEM((inner, slots, lines, lanes), jnp.float32)] * steps
        + [
            pltpu.SemaphoreType.DMA((steps,)),
            pltpu.SemaphoreType.DMA((steps,)),
            pltpu.SemaphoreType.DMA((2,)),
            pltpu.SemaphoreType.DMA((steps * inner,)),
            pltpu.SemaphoreType.DMA((steps * inner,)),
            pltpu.SemaphoreType.DMA((steps,)),
            pltpu.VMEM((planes, *tile), jnp.float32),
            pltpu.VMEM((inner, planes, *tile), jnp.float32),
            pltpu.VMEM((groups, inner, planes, *tile), jnp.float32),
            pltpu.SemaphoreType.DMA((hops,)),
            pltpu.SemaphoreType.DMA((hops,)),
            pltpu.SemaphoreType.DMA((2,)),
        ],
        cost_estimate=pl.CostEstimate(flops=0, bytes_accessed=sent * 4, transcendentals=0),
        compiler_params=pltpu.CompilerParams(
            collective_id=branch, has_side_effects=True, vmem_limit_bytes=60 * 1024 * 1024
        ),
    )(positions, sums, master_send, update_send)


def shards(master, first_moment, second_moment, rotation, assignment):
    dp_count = lax.axis_size("dp")
    group_count = lax.axis_size("expert")
    position = lax.axis_index("dp")
    round_count = rotation.shape[0]
    rows_here = master.shape[1]
    lane_count = LANE
    per_row = master.shape[2] // lane_count
    lines_device = rows_here * per_row
    piece_len = lines_device // (round_count * dp_count)
    inv_count = 1.0 / math.sqrt(dp_count * piece_len * lane_count)
    table = slot_table(rotation, dp_count, MOST)
    span_count = round_count * dp_count
    inner = INNER
    planes = dp_count // inner
    slots = round_count * MOST

    plane_of = rotation.reshape(span_count) // inner
    span_ids = jnp.arange(span_count, dtype=jnp.int32)
    same = (plane_of[:, None] == plane_of[None, :]) & (span_ids[None, :] < span_ids[:, None])
    place_of = jnp.sum(same.astype(jnp.int32), axis=1)
    plane_ids = jnp.arange(planes, dtype=jnp.int32)
    loads = jnp.sum((plane_of[None, :] == plane_ids[:, None]).astype(jnp.int32), axis=1)
    most_load = jnp.max(loads)
    cap_all = min(inner * slots, span_count)
    mean_load = span_count // planes
    caps = sorted({min(cap_all, mean_load * eighths // 8) for eighths in (10, 11, 12, 13, 14, 16)} | {cap_all})
    choice = sum((most_load > cap).astype(jnp.int32) for cap in caps[:-1])
    place_ids = jnp.arange(cap_all, dtype=jnp.int32)
    listed = (plane_of[None, None, :] == plane_ids[:, None, None]) & (
        place_of[None, None, :] == place_ids[None, :, None]
    )
    lists = jnp.sum(listed.astype(jnp.int32) * span_ids, axis=2)
    mine = table.transpose(2, 0, 1).reshape(planes, inner, round_count, MOST)
    mine = lax.dynamic_index_in_dim(mine, position // inner, 0, keepdims=False)
    padded_place = jnp.concatenate(
        [place_of.reshape(round_count, dp_count), jnp.full((round_count, 1), cap_all, jnp.int32)], axis=1
    )
    hits = mine[..., None] == jnp.arange(dp_count + 1, dtype=jnp.int32)
    positions = jnp.sum(hits * padded_place[None, :, None, :], axis=3).reshape(inner, slots)

    update = scaled_moment(first_moment, second_moment)
    master_lines = master.reshape(span_count, piece_len, lane_count)
    update_lines = update.reshape(span_count, piece_len, lane_count)
    local_lines = position * lines_device + jnp.arange(lines_device, dtype=jnp.int32).reshape(
        span_count, piece_len
    )
    weights = position_weights(local_lines, per_row, lane_count)
    master_sums = jnp.sum(master_lines * weights, axis=(1, 2)) * inv_count
    update_sums = jnp.sum(update_lines * weights, axis=(1, 2)) * inv_count

    permuting = (assignment[:, None] == span_ids[None, :]).astype(jnp.float32)
    both_sums = jnp.stack([master_sums, update_sums])
    placed_sums = jnp.sum(both_sums[:, :, None] * permuting[None], axis=1)
    entries = 2 * span_count
    tile_size = 8 * lane_count
    sums = jnp.pad(placed_sums.reshape(entries), (0, -entries % tile_size)).reshape(-1, lane_count)

    def branch_of(number, cap):
        def run(master_in, update_in):
            chosen = lists[:, :cap]
            return exchange(
                planes,
                inner,
                group_count,
                slots,
                cap,
                number,
                positions,
                sums,
                master_in[chosen],
                update_in[chosen],
            )

        return run

    saved_master, saved_update, totals = lax.switch(
        choice, [branch_of(number, cap) for number, cap in enumerate(caps)], master_lines, update_lines
    )
    checksums = totals.reshape(group_count, -1)[:, :entries].reshape(group_count, 2, span_count)
    shape_out = (1, round_count, MOST, dp_count * piece_len, lane_count)
    return (saved_master.reshape(shape_out), saved_update.reshape(shape_out), checksums)


def solution(mesh):
    placed = (P("expert", "dp", None), P("expert", "dp", None), P("expert", "dp", None), P(), P())
    return jax.shard_map(
        shards,
        mesh=mesh,
        in_specs=placed,
        out_specs=(P("expert", "dp", None, None, None), P("expert", "dp", None, None, None), P()),
        check_vma=False,
    )
```
